32 devices in a mesh: freq: 4 (over y, x), shot: 8 (over z, core).
Axes of the slice: x: 2, y: 2, z: 4, core: 2. Of those that a mesh axis runs over, the one named last changes fastest.
Arguments:
- traces: bfloat16 [2, 4, 3072, 3072], P(None, 'freq', 'shot'), may hold values from -40 to 40, as said below
Outputs:
- multiples: bfloat16 [2, 4, 3072, 3072], P(None, 'freq', 'shot')
- primaries: bfloat16 [2, 4, 3072, 3072], P(None, 'freq', 'shot')
The draws below stay inside these ranges and needn't reach their ends.
Inputs may be any that keep to these rules, and one draw needn't show every extreme that they name: `traces`: finite recorded data.
All inputs are finite; a program needn't handle non-finite values.
Results may differ from the reference program's by a relative error of at most 0.0005.
Values may be sent and summed in bfloat16 or wider, within the bound.
A program may use at most 192 MiB of HBM per device.

```python
import math
import jax
import jax.numpy as jnp
from jax import lax

NRECV = 3072
FREQS = 4


def draw_traces(key, part):
    row_index = jnp.arange(NRECV, dtype=jnp.float32)
    row_ramp = jnp.sqrt(1.0 + 2.0 * row_index / (NRECV - 1))

    def per_band(freq_index):
        band_key = jax.random.fold_in(key, freq_index + 17)
        noise_key, scale_key = jax.random.split(band_key)
        noise = jnp.clip(jax.random.normal(noise_key, (2, NRECV, NRECV), jnp.float32), -4.0, 4.0)
        row_scale = jnp.exp(jax.random.uniform(scale_key, (NRECV,), jnp.float32, math.log(0.4), math.log(4.0)))
        base = noise * (0.3 * 0.70710678 * row_scale * row_ramp)[None, :, None]
        base_re = base[0]
        base_im = base[1]
        square_re = jnp.dot(base_re, base_re, precision=lax.Precision.HIGHEST) - jnp.dot(base_im, base_im, precision=lax.Precision.HIGHEST)
        square_im = jnp.dot(base_re, base_im, precision=lax.Precision.HIGHEST) + jnp.dot(base_im, base_re, precision=lax.Precision.HIGHEST)
        amplitude = 1.0 + 0.35 * freq_index.astype(jnp.float32) / (FREQS - 1)
        factor = 0.5 / math.sqrt(NRECV)
        return amplitude * jnp.stack([base_re + factor * square_re, base_im + factor * square_im])
    stacked = lax.map(per_band, jnp.arange(FREQS))
    return jnp.clip(jnp.transpose(stacked, (1, 0, 2, 3)), -40.0, 40.0).astype(jnp.bfloat16)


def setup_inputs(seed: int = 0) -> dict:
    seeds = jax.random.split(jax.random.key(seed), 2)
    traces = draw_traces(jax.random.fold_in(seeds[1], 71), 0)
    return dict(traces=traces)


epsilon = 1e-06

def reference(traces):
    factor = 1.0 / math.sqrt(NRECV)
    data = traces.astype(jnp.float32)

    def per_band(freq_index):
        data_re = data[0, freq_index]
        data_im = data[1, freq_index]
        mult_re = (jnp.dot(data_re, data_re, precision=lax.Precision.HIGHEST) - jnp.dot(data_im, data_im, precision=lax.Precision.HIGHEST)) * factor
        mult_im = (jnp.dot(data_re, data_im, precision=lax.Precision.HIGHEST) + jnp.dot(data_im, data_re, precision=lax.Precision.HIGHEST)) * factor
        return jnp.stack([mult_re, mult_im])
    mult = lax.map(per_band, jnp.arange(FREQS))
    mult = jnp.transpose(mult, (1, 0, 2, 3))
    mult_re = mult[0]
    mult_im = mult[1]
    data_re = data[0]
    data_im = data[1]
    total_count = float(FREQS * NRECV * NRECV)
    num_re = jnp.sum(mult_re * data_re + mult_im * data_im) / total_count
    num_im = jnp.sum(mult_re * data_im - mult_im * data_re) / total_count
    denom = jnp.sum(mult_re * mult_re + mult_im * mult_im) / total_count + epsilon
    fit_re = num_re / denom
    fit_im = num_im / denom
    prim_re = data_re - (fit_re * mult_re - fit_im * mult_im)
    prim_im = data_im - (fit_re * mult_im + fit_im * mult_re)
    primaries = jnp.stack([prim_re, prim_im]).astype(jnp.bfloat16)
    return (mult.astype(jnp.bfloat16), primaries)
```

```python
import functools
import math

import jax
import jax.numpy as jnp
from jax import lax
from jax.experimental import pallas as pl
from jax.experimental.pallas import tpu as pltpu
from jax.sharding import PartitionSpec as P

epsilon = 1e-06
MESH = pl.DeviceIdType.MESH


def complex_product(left_re, left_im, right):
    left_block = jnp.stack(
        [jnp.concatenate([left_re, -left_im], axis=2), jnp.concatenate([left_im, left_re], axis=2)]
    )
    right_block = jnp.concatenate([right[0], right[1]], axis=1)
    return jnp.einsum("cfik,fkn->cfin", left_block, right_block, preferred_element_type=jnp.float32)


def finish(traces, mult_re, mult_im, num_re, num_im, denom):
    matrix_order = traces.shape[3]
    data_re = traces[0].astype(jnp.float32)
    data_im = traces[1].astype(jnp.float32)
    total_count = float(traces.shape[1] * lax.axis_size("freq") * matrix_order * matrix_order)
    scaled_den = denom / total_count + epsilon
    fit_re = num_re / total_count / scaled_den
    fit_im = num_im / total_count / scaled_den
    prim_re = data_re - (fit_re * mult_re - fit_im * mult_im)
    prim_im = data_im - (fit_re * mult_im + fit_im * mult_re)
    multiples = jnp.stack([mult_re, mult_im]).astype(jnp.bfloat16)
    primaries = jnp.stack([prim_re, prim_im]).astype(jnp.bfloat16)
    return (multiples, primaries)


def gathered(traces):
    factor = 1.0 / math.sqrt(traces.shape[3])
    products = complex_product(
        traces[0], traces[1], lax.all_gather(traces, "shot", axis=2, tiled=True)
    )
    mult_re = products[0] * factor
    mult_im = products[1] * factor
    data_re = traces[0].astype(jnp.float32)
    data_im = traces[1].astype(jnp.float32)
    sums = lax.psum(
        jnp.stack([
            jnp.sum(mult_re * data_re + mult_im * data_im),
            jnp.sum(mult_re * data_im - mult_im * data_re),
            jnp.sum(mult_re * mult_re + mult_im * mult_im),
        ]),
        ("freq", "shot"),
    )
    return finish(traces, mult_re, mult_im, sums[0], sums[1], sums[2])


def line_kernel(
    chunks, kept, width, step, freqs, shots,
    traces_ref, mult_ref, total_ref,
    grid, own_stage, help_stage, acc, sums,
    load_sem, out_sem, ici_recv, pair_recv, far_send, end_send, pair_send,
    result_send, result_recv, sum_send, sum_recv,
):
    rows = traces_ref.shape[1]
    order = traces_ref.shape[2]
    factor = 1.0 / math.sqrt(order)
    freq = lax.axis_index("freq")
    shot = lax.axis_index("shot")
    z = shot // 2
    core = shot % 2
    low = z < 2
    end = jnp.where(low, 0, 3)
    mid = jnp.where(low, 1, 2)
    far_mid = jnp.where(low, 2, 1)
    far_end = jnp.where(low, 3, 0)
    is_end = z == end

    def block(chip, plane, j):
        first = pl.multiple_of((chip * 2 + plane) * rows, rows)
        return grid.at[:, pl.ds(first, rows), pl.ds(pl.multiple_of(j * width, width), width)]

    def remote(src, dst, send, recv, chip, plane):
        return pltpu.make_async_remote_copy(
            src_ref=src, dst_ref=dst, send_sem=send, recv_sem=recv,
            device_id=(freq, chip * 2 + plane), device_id_type=MESH,
        )

    def ici(chip, j, send, slot, target):
        ref = block(chip, core, j)
        return remote(ref, ref, send, ici_recv.at[slot, j], target, core)

    def pair(chip, j, slot):
        ref = block(chip, core, j)
        return remote(ref, ref, pair_send.at[slot, j], pair_recv.at[slot, j], z, 1 - core)

    def arrived(chip, j, slot):
        ref = block(chip, core, j)
        remote(ref, ref, far_send.at[0, j], ici_recv.at[slot, j], z, 1 - core).wait_recv()

    def paired(chip, j, slot):
        ref = block(chip, 1 - core, j)
        remote(ref, ref, pair_send.at[slot, j], pair_recv.at[slot, j], z, 1 - core).wait_recv()

    def to_end(chip, j, slot):
        return ici(chip, j, end_send.at[slot, j], slot, end)

    def to_far(chip, j, slot):
        return ici(chip, j, far_send.at[slot, j], slot + 1, far_mid)

    def to_mid(j):
        return ici(z, j, end_send.at[0, j], 0, mid)

    def own_out(j, s):
        return pltpu.make_async_copy(
            own_stage.at[s],
            mult_ref.at[:, :, pl.ds(pl.multiple_of(j * width, width), width)],
            out_sem.at[s],
        )

    def result(j, s):
        return remote(
            help_stage.at[s],
            mult_ref.at[:, :, pl.ds(pl.multiple_of(j * width, width), width)],
            result_send.at[s], result_recv.at[j], end, core,
        )

    def multiply(chip, j, stage, s):
        first = pl.multiple_of((chip * 2 + core) * rows, rows)

        def part(q, carry):
            column = pl.multiple_of(j * width + q * step, step)
            left_re = grid[0, pl.ds(first, rows), :]
            left_im = grid[1, pl.ds(first, rows), :]
            right_re = grid[0, :, pl.ds(column, step)]
            right_im = grid[1, :, pl.ds(column, step)]
            dot = functools.partial(jnp.dot, preferred_element_type=jnp.float32)
            mult_re = (dot(left_re, right_re) - dot(left_im, right_im)) * factor
            mult_im = (dot(left_re, right_im) + dot(left_im, right_re)) * factor
            here = pl.ds(pl.multiple_of(q * step, step), step)
            stage[s, 0, :, here] = mult_re
            stage[s, 1, :, here] = mult_im
            data_re = grid[0, pl.ds(first, rows), pl.ds(column, step)].astype(jnp.float32)
            data_im = grid[1, pl.ds(first, rows), pl.ds(column, step)].astype(jnp.float32)
            for i, term in enumerate((
                mult_re * data_re + mult_im * data_im,
                mult_re * data_im - mult_im * data_re,
                mult_re * mult_re + mult_im * mult_im,
            )):
                folded = jnp.sum(term.reshape(rows // 8, 8, step), axis=0)
                lanes = folded[:, :128]
                for k in range(1, step // 128):
                    lanes = lanes + folded[:, k * 128:(k + 1) * 128]
                acc[pl.ds(i * 8, 8), :] += lanes
            return carry

        lax.fori_loop(0, width // step, part, 0)

    acc[...] = jnp.zeros_like(acc)
    mine = grid.at[:, pl.ds(pl.multiple_of(shot * rows, rows), rows), :]
    load = pltpu.make_async_copy(traces_ref, mine, load_sem)
    load.start()
    load.wait()

    def loop(lower, upper, body):
        def run(j, carry):
            body(j)
            return carry
        lax.fori_loop(lower, upper, run, 0)

    @pl.when(is_end)
    def _():
        def first_sends(j):
            to_mid(j).start()

            @pl.when(j < kept)
            def _():
                pair(z, j, 3).start()

        loop(0, chunks, first_sends)

        def work(j):
            for slot, chip in enumerate((mid, far_mid, far_end)):
                arrived(chip, j, slot)
                pair(chip, j, slot).start()
            for slot, chip in enumerate((mid, far_mid, far_end, end)):
                paired(chip, j, slot)
            s = j % 2

            @pl.when(j >= 2)
            def _():
                own_out(j - 2, s).wait()
            multiply(z, j, own_stage, s)
            own_out(j, s).start()

        loop(0, kept, work)
        loop(kept - 2, kept, lambda j: own_out(j, j % 2).wait())

        def drain(j):
            to_mid(j).wait_send()

            @pl.when(j < kept)
            def _():
                for slot, chip in enumerate((mid, far_mid, far_end, end)):
                    pair(chip, j, slot).wait_send()

        loop(0, chunks, drain)

    @pl.when(jnp.logical_not(is_end))
    def _():
        def own_sends(j):
            to_far(z, j, 0).start()

            @pl.when(j < kept)
            def _():
                to_end(z, j, 0).start()
            pair(z, j, 3).start()

        def near(j):
            arrived(end, j, 0)
            to_far(end, j, 1).start()
            pair(end, j, 0).start()

        ahead = 2
        loop(0, ahead, own_sends)
        loop(0, ahead, near)

        def work(j):
            upper = jnp.where(j < kept, jnp.minimum(j + ahead + 1, chunks), chunks)
            lower = jnp.where(j <= kept, jnp.minimum(j + ahead, chunks), chunks)

            def more(jj):
                own_sends(jj)
                near(jj)

            loop(lower, upper, more)
            for slot, chip in ((1, far_mid), (2, far_end)):
                arrived(chip, j, slot)

                @pl.when(j < kept)
                def _():
                    to_end(chip, j, slot).start()
                pair(chip, j, slot).start()
            for slot, chip in enumerate((end, far_mid, far_end, z)):
                paired(chip, j, slot)
            s = j % 2

            @pl.when(j >= kept)
            def _():
                @pl.when(j >= kept + 2)
                def _():
                    result(j - 2, s).wait_send()
                multiply(end, j, help_stage, s)
                result(j, s).start()

            @pl.when(j >= 2)
            def _():
                own_out(j - 2, s).wait()
            multiply(z, j, own_stage, s)
            own_out(j, s).start()

        loop(0, chunks, work)

        def drain(j):
            to_far(z, j, 0).wait_send()
            to_far(end, j, 1).wait_send()
            for slot, chip in enumerate((end, far_mid, far_end, z)):
                pair(chip, j, slot).wait_send()

            @pl.when(j < kept)
            def _():
                for slot, chip in enumerate((z, far_mid, far_end)):
                    to_end(chip, j, slot).wait_send()

        loop(0, chunks, drain)

    devices = freqs * shots
    me = freq * shots + shot

    def give(d):
        target = (me + d) % devices
        return pltpu.make_async_remote_copy(
            src_ref=acc, dst_ref=sums.at[d - 1],
            send_sem=sum_send.at[d - 1], recv_sem=sum_recv.at[d - 1],
            device_id=(target // shots, target % shots), device_id_type=MESH,
        )

    loop(1, devices, lambda d: give(d).start())
    loop(1, devices, lambda d: give(d).wait_recv())
    total_ref[...] = acc[...] + jnp.sum(sums[...], axis=0)

    @pl.when(is_end)
    def _():
        loop(kept, chunks, lambda j: result(j, 0).wait_recv())

    @pl.when(jnp.logical_not(is_end))
    def _():
        def last(j):
            own_out(j, j % 2).wait()
            result(j, j % 2).wait_send()
        loop(chunks - 2, chunks, last)

    loop(1, devices, lambda d: give(d).wait_send())


def on_a_line(traces):
    rows, order = traces.shape[2], traces.shape[3]
    freqs, shots = lax.axis_size("freq"), lax.axis_size("shot")
    step = 256
    width = step
    chunks = order // width
    kept = chunks // 3
    devices = freqs * shots
    dma = pltpu.SemaphoreType.DMA
    mult, totals = pl.pallas_call(
        functools.partial(line_kernel, chunks, kept, width, step, freqs, shots),
        out_shape=(
            jax.ShapeDtypeStruct((2, rows, order), jnp.float32),
            jax.ShapeDtypeStruct((24, 128), jnp.float32),
        ),
        in_specs=[pl.BlockSpec(memory_space=pl.ANY)],
        out_specs=(
            pl.BlockSpec(memory_space=pl.ANY),
            pl.BlockSpec(memory_space=pltpu.VMEM),
        ),
        scratch_shapes=[
            pltpu.VMEM((2, order, order), jnp.bfloat16),
            pltpu.VMEM((2, 2, rows, width), jnp.float32),
            pltpu.VMEM((2, 2, rows, width), jnp.float32),
            pltpu.VMEM((24, 128), jnp.float32),
            pltpu.VMEM((devices - 1, 24, 128), jnp.float32),
            dma, dma((2,)), dma((3, chunks)), dma((4, chunks)), dma((2, chunks)),
            dma((3, chunks)), dma((4, chunks)),
            dma((2,)), dma((chunks,)), dma((devices - 1,)), dma((devices - 1,)),
        ],
        compiler_params=pltpu.CompilerParams(
            has_side_effects=True, vmem_limit_bytes=60 * 1024 * 1024
        ),
    )(traces[:, 0])
    sums = jnp.sum(totals.reshape(3, 8 * 128), axis=1)
    return finish(traces, mult[0][None], mult[1][None], sums[0], sums[1], sums[2])


def solution(mesh):
    placed = P(None, "freq", "shot", None)

    def per_device(traces):
        four_chips = mesh.shape["shot"] == 2 * 4
        if four_chips and traces.shape[1] == 1 and traces.shape[3] % 256 == 0:
            return on_a_line(traces)
        return gathered(traces)

    return jax.shard_map(
        per_device, mesh=mesh, in_specs=(placed,), out_specs=(placed, placed), check_vma=False
    )
```

```python
import functools
import math

import jax
import jax.numpy as jnp
from jax import lax
from jax.experimental import pallas as pl
from jax.experimental.pallas import tpu as pltpu
from jax.sharding import PartitionSpec as P

epsilon = 1e-06
MESH = pl.DeviceIdType.MESH


def complex_product(left_re, left_im, right):
    left_block = jnp.stack(
        [jnp.concatenate([left_re, -left_im], axis=2), jnp.concatenate([left_im, left_re], axis=2)]
    )
    right_block = jnp.concatenate([right[0], right[1]], axis=1)
    return jnp.einsum("cfik,fkn->cfin", left_block, right_block, preferred_element_type=jnp.float32)


def finish(traces, mult_re, mult_im, num_re, num_im, denom):
    matrix_order = traces.shape[3]
    data_re = traces[0].astype(jnp.float32)
    data_im = traces[1].astype(jnp.float32)
    total_count = float(traces.shape[1] * lax.axis_size("freq") * matrix_order * matrix_order)
    scaled_den = denom / total_count + epsilon
    fit_re = num_re / total_count / scaled_den
    fit_im = num_im / total_count / scaled_den
    prim_re = data_re - (fit_re * mult_re - fit_im * mult_im)
    prim_im = data_im - (fit_re * mult_im + fit_im * mult_re)
    multiples = jnp.stack([mult_re, mult_im]).astype(jnp.bfloat16)
    primaries = jnp.stack([prim_re, prim_im]).astype(jnp.bfloat16)
    return (multiples, primaries)


def gathered(traces):
    factor = 1.0 / math.sqrt(traces.shape[3])
    products = complex_product(
        traces[0], traces[1], lax.all_gather(traces, "shot", axis=2, tiled=True)
    )
    mult_re = products[0] * factor
    mult_im = products[1] * factor
    data_re = traces[0].astype(jnp.float32)
    data_im = traces[1].astype(jnp.float32)
    sums = lax.psum(
        jnp.stack([
            jnp.sum(mult_re * data_re + mult_im * data_im),
            jnp.sum(mult_re * data_im - mult_im * data_re),
            jnp.sum(mult_re * mult_re + mult_im * mult_im),
        ]),
        ("freq", "shot"),
    )
    return finish(traces, mult_re, mult_im, sums[0], sums[1], sums[2])


def line_kernel(
    chunks, kept, width, step, freqs, shots,
    traces_ref, mult_ref, total_ref,
    grid, help_stage, acc, sums,
    load_sem, ici_recv, pair_recv, far_send, end_send, pair_send,
    result_send, result_recv, sum_send, sum_recv,
):
    rows = traces_ref.shape[2]
    order = traces_ref.shape[3]
    factor = 1.0 / math.sqrt(order)
    freq = lax.axis_index("freq")
    shot = lax.axis_index("shot")
    z = shot // 2
    core = shot % 2
    low = z < 2
    end = jnp.where(low, 0, 3)
    mid = jnp.where(low, 1, 2)
    far_mid = jnp.where(low, 2, 1)
    far_end = jnp.where(low, 3, 0)
    is_end = z == end

    def block(chip, plane, j):
        first = pl.multiple_of((chip * 2 + plane) * rows, rows)
        return grid.at[:, pl.ds(first, rows), pl.ds(pl.multiple_of(j * width, width), width)]

    def remote(src, dst, send, recv, chip, plane):
        return pltpu.make_async_remote_copy(
            src_ref=src, dst_ref=dst, send_sem=send, recv_sem=recv,
            device_id=(freq, chip * 2 + plane), device_id_type=MESH,
        )

    def ici(chip, j, send, slot, target):
        ref = block(chip, core, j)
        return remote(ref, ref, send, ici_recv.at[slot, j], target, core)

    def pair(chip, j, slot):
        ref = block(chip, core, j)
        return remote(ref, ref, pair_send.at[slot, j], pair_recv.at[slot, j], z, 1 - core)

    def arrived(chip, j, slot):
        ref = block(chip, core, j)
        remote(ref, ref, far_send.at[0, j], ici_recv.at[slot, j], z, 1 - core).wait_recv()

    def paired(chip, j, slot):
        ref = block(chip, 1 - core, j)
        remote(ref, ref, pair_send.at[slot, j], pair_recv.at[slot, j], z, 1 - core).wait_recv()

    def to_end(chip, j, slot):
        return ici(chip, j, end_send.at[slot, j], slot, end)

    def to_far(chip, j, slot):
        return ici(chip, j, far_send.at[slot, j], slot + 1, far_mid)

    def to_mid(j):
        return ici(z, j, end_send.at[0, j], 0, mid)

    def result(j, s):
        return remote(
            help_stage.at[s],
            mult_ref.at[:, :, pl.ds(pl.multiple_of(j * width, width), width)],
            result_send.at[s], result_recv.at[j], end, core,
        )

    def multiply(chip, j, stage, start):
        first = pl.multiple_of((chip * 2 + core) * rows, rows)

        def part(q, carry):
            column = pl.multiple_of(j * width + q * step, step)
            left_re = grid[0, pl.ds(first, rows), :]
            left_im = grid[1, pl.ds(first, rows), :]
            right_re = grid[0, :, pl.ds(column, step)]
            right_im = grid[1, :, pl.ds(column, step)]
            dot = functools.partial(jnp.dot, preferred_element_type=jnp.float32)
            mult_re = (dot(left_re, right_re) - dot(left_im, right_im)) * factor
            mult_im = (dot(left_re, right_im) + dot(left_im, right_re)) * factor
            here = pl.ds(pl.multiple_of(start + q * step, step), step)
            stage[0, :, here] = mult_re
            stage[1, :, here] = mult_im
            data_re = grid[0, pl.ds(first, rows), pl.ds(column, step)].astype(jnp.float32)
            data_im = grid[1, pl.ds(first, rows), pl.ds(column, step)].astype(jnp.float32)
            for i, term in enumerate((
                mult_re * data_re + mult_im * data_im,
                mult_re * data_im - mult_im * data_re,
                mult_re * mult_re + mult_im * mult_im,
            )):
                folded = jnp.sum(term.reshape(rows // 8, 8, step), axis=0)
                lanes = folded[:, :128]
                for k in range(1, step // 128):
                    lanes = lanes + folded[:, k * 128:(k + 1) * 128]
                acc[pl.ds(i * 8, 8), :] += lanes
            return carry

        lax.fori_loop(0, width // step, part, 0)

    acc[...] = jnp.zeros_like(acc)
    mine = grid.at[:, pl.ds(pl.multiple_of(shot * rows, rows), rows), :]
    load = pltpu.make_async_copy(traces_ref.at[:, 0], mine, load_sem)
    load.start()
    load.wait()

    def loop(lower, upper, body):
        def run(j, carry):
            body(j)
            return carry
        lax.fori_loop(lower, upper, run, 0)

    @pl.when(is_end)
    def _():
        def first_sends(j):
            to_mid(j).start()

            @pl.when(j < kept)
            def _():
                pair(z, j, 3).start()

        loop(0, chunks, first_sends)

        def work(j):
            for slot, chip in enumerate((mid, far_mid, far_end)):
                arrived(chip, j, slot)
                pair(chip, j, slot).start()
            for slot, chip in enumerate((mid, far_mid, far_end, end)):
                paired(chip, j, slot)
            multiply(z, j, mult_ref, j * width)

        loop(0, kept, work)

        def drain(j):
            to_mid(j).wait_send()

            @pl.when(j < kept)
            def _():
                for slot, chip in enumerate((mid, far_mid, far_end, end)):
                    pair(chip, j, slot).wait_send()

        loop(0, chunks, drain)

    @pl.when(jnp.logical_not(is_end))
    def _():
        def own_sends(j):
            to_far(z, j, 0).start()

            @pl.when(j < kept)
            def _():
                to_end(z, j, 0).start()
            pair(z, j, 3).start()

        def near(j):
            arrived(end, j, 0)
            to_far(end, j, 1).start()
            pair(end, j, 0).start()

        ahead = 2
        loop(0, ahead, own_sends)
        loop(0, ahead, near)

        def work(j):
            for slot, chip in ((1, far_mid), (2, far_end)):
                arrived(chip, j, slot)

                @pl.when(j < kept)
                def _():
                    to_end(chip, j, slot).start()
                pair(chip, j, slot).start()
            for slot, chip in ((1, far_mid), (2, far_end), (3, z)):
                paired(chip, j, slot)
            upper = jnp.where(j < kept, jnp.minimum(j + ahead + 1, chunks), chunks)
            lower = jnp.where(j <= kept, jnp.minimum(j + ahead, chunks), chunks)

            def more(jj):
                own_sends(jj)
                near(jj)

            loop(lower, upper, more)
            paired(end, j, 0)
            s = j % 2

            @pl.when(j >= kept)
            def _():
                @pl.when(j >= kept + 2)
                def _():
                    result(j - 2, s).wait_send()
                multiply(end, j, help_stage.at[s], 0)
                result(j, s).start()

            multiply(z, j, mult_ref, j * width)

        loop(0, chunks, work)

        def drain(j):
            to_far(z, j, 0).wait_send()
            to_far(end, j, 1).wait_send()
            for slot, chip in enumerate((end, far_mid, far_end, z)):
                pair(chip, j, slot).wait_send()

            @pl.when(j < kept)
            def _():
                for slot, chip in enumerate((z, far_mid, far_end)):
                    to_end(chip, j, slot).wait_send()

        loop(0, chunks, drain)

    devices = freqs * shots
    me = freq * shots + shot

    def give(d):
        target = (me + d) % devices
        return pltpu.make_async_remote_copy(
            src_ref=acc, dst_ref=sums.at[d - 1],
            send_sem=sum_send.at[d - 1], recv_sem=sum_recv.at[d - 1],
            device_id=(target // shots, target % shots), device_id_type=MESH,
        )

    loop(1, devices, lambda d: give(d).start())
    loop(1, devices, lambda d: give(d).wait_recv())
    total_ref[...] = acc[...] + jnp.sum(sums[...], axis=0)

    @pl.when(is_end)
    def _():
        loop(kept, chunks, lambda j: result(j, 0).wait_recv())

    @pl.when(jnp.logical_not(is_end))
    def _():
        def last(j):
            result(j, j % 2).wait_send()
        loop(chunks - 2, chunks, last)

    loop(1, devices, lambda d: give(d).wait_send())


def epilogue_kernel(total_count, total_ref, traces_ref, mult_ref, multiples_ref, primaries_ref, fit):
    @pl.when(pl.program_id(0) == 0)
    def _():
        num_re, num_im, denom = (jnp.sum(total_ref[pl.ds(8 * i, 8), :]) for i in range(3))
        scaled_den = denom / total_count + epsilon
        fit[0] = num_re / total_count / scaled_den
        fit[1] = num_im / total_count / scaled_den

    fit_re = fit[0]
    fit_im = fit[1]
    strip = traces_ref.shape[2]
    first = pl.multiple_of(pl.program_id(0) * strip, strip)
    mult_re = mult_ref[0, pl.ds(first, strip), :]
    mult_im = mult_ref[1, pl.ds(first, strip), :]
    data_re = traces_ref[0, 0].astype(jnp.float32)
    data_im = traces_ref[1, 0].astype(jnp.float32)
    prim_re = data_re - (fit_re * mult_re - fit_im * mult_im)
    prim_im = data_im - (fit_re * mult_im + fit_im * mult_re)
    multiples_ref[0, 0] = mult_re.astype(jnp.bfloat16)
    multiples_ref[1, 0] = mult_im.astype(jnp.bfloat16)
    primaries_ref[0, 0] = prim_re.astype(jnp.bfloat16)
    primaries_ref[1, 0] = prim_im.astype(jnp.bfloat16)


def on_a_line(traces):
    rows, order = traces.shape[2], traces.shape[3]
    freqs, shots = lax.axis_size("freq"), lax.axis_size("shot")
    step = 256
    width = step
    chunks = order // width
    kept = chunks // 3
    devices = freqs * shots
    dma = pltpu.SemaphoreType.DMA
    mult, totals = pl.pallas_call(
        functools.partial(line_kernel, chunks, kept, width, step, freqs, shots),
        out_shape=(
            pltpu.VMEM((2, rows, order), jnp.float32),
            jax.ShapeDtypeStruct((24, 128), jnp.float32),
        ),
        in_specs=[pl.BlockSpec(memory_space=pltpu.HBM)],
        out_specs=(
            pl.BlockSpec(memory_space=pltpu.VMEM),
            pl.BlockSpec(memory_space=pltpu.VMEM),
        ),
        scratch_shapes=[
            pltpu.VMEM((2, order, order), jnp.bfloat16),
            pltpu.VMEM((2, 2, rows, width), jnp.float32),
            pltpu.VMEM((24, 128), jnp.float32),
            pltpu.VMEM((devices - 1, 24, 128), jnp.float32),
            dma, dma((3, chunks)), dma((4, chunks)), dma((2, chunks)),
            dma((3, chunks)), dma((4, chunks)),
            dma((2,)), dma((chunks,)), dma((devices - 1,)), dma((devices - 1,)),
        ],
        compiler_params=pltpu.CompilerParams(
            has_side_effects=True, vmem_limit_bytes=48 * 1024 * 1024
        ),
    )(traces)
    strip = rows // 12 if rows % (12 * 16) == 0 else rows
    block = pl.BlockSpec((2, 1, strip, order), lambda i: (0, 0, i, 0))
    out = jax.ShapeDtypeStruct(traces.shape, traces.dtype)
    return pl.pallas_call(
        functools.partial(epilogue_kernel, float(freqs * order * order)),
        grid=(rows // strip,),
        out_shape=(out, out),
        in_specs=[
            pl.BlockSpec((24, 128), lambda i: (0, 0)),
            block,
            pl.BlockSpec(memory_space=pltpu.VMEM),
        ],
        out_specs=(block, block),
        scratch_shapes=[pltpu.SMEM((2,), jnp.float32)],
        compiler_params=pltpu.CompilerParams(
            dimension_semantics=("arbitrary",), vmem_limit_bytes=24 * 1024 * 1024
        ),
    )(totals, traces, mult)


def solution(mesh):
    placed = P(None, "freq", "shot", None)

    def per_device(traces):
        four_chips = mesh.shape["shot"] == 2 * 4
        if four_chips and traces.shape[1] == 1 and traces.shape[3] % 256 == 0:
            return on_a_line(traces)
        return gathered(traces)

    return jax.shard_map(
        per_device, mesh=mesh, in_specs=(placed,), out_specs=(placed, placed), check_vma=False
    )
```
